32 devices in a mesh: ha: 4 (over z), wa: 4 (over y, core), hd: 2 (over x).
Axes of the slice: x: 2, y: 2, z: 4, core: 2. Of those that a mesh axis runs over, the one named last changes fastest.
Arguments:
- queries: bfloat16 [12, 32, 64, 3072], P(None, 'ha', 'wa', 'hd'), may hold values from -10 to 10
- video_keys: bfloat16 [12, 32, 64, 3072], P(None, 'ha', 'wa', 'hd'), may hold values from -5 to 5
- video_values: bfloat16 [12, 32, 64, 3072], P(None, 'ha', 'wa', 'hd'), may hold values from -6 to 6
- text_keys: bfloat16 [256, 3072], P(None, 'hd'), may hold values from -5 to 5
- text_values: bfloat16 [256, 3072], P(None, 'hd'), may hold values from -6 to 6
- tile_radius: int32 [3, 2, 4, 8], P(None, None, 'ha', 'wa'), may hold values from 0 to 1, as said below
- out_weight: bfloat16 [3072, 3072], P('hd'), may hold values from -0.875 to 0.875
Outputs:
- projected: bfloat16 [12, 32, 64, 3072], P(None, 'ha', 'wa', 'hd')
The draws below stay inside these ranges and needn't reach their ends.
Inputs may be any that keep to these rules, and one draw needn't show every extreme that they name: `tile_radius`: every video query has a window of at most one tile in each direction; some tile has radius 1 in all three.
All inputs are finite; a program needn't handle non-finite values.
Results may differ from the reference program's by a relative error of at most 0.012.
Values may be sent and summed in bfloat16 or wider, within the bound.
A program may use at most 256 MiB of HBM per device.

```python
import jax
import jax.numpy as jnp
from jax import lax

HEADS = 24
HEAD = 128
D = 3072
TEXT = 256
TILE_T = 6
TILE_H = 8
TILE_W = 8
TT_TILES = 2
FRAMES = 12
ROW_TILES = 4
COL_TILES = 8
HEIGHT = 32
WIDTH = 64
N_HD = 2


def paired_draw(key):
    base = jax.random.fold_in(key, 71)
    shape = (FRAMES, HEIGHT, WIDTH, HEADS * HEAD)
    first = jax.random.normal(jax.random.fold_in(base, 1), shape, jnp.float32)
    second = jax.random.normal(jax.random.fold_in(base, 2), shape, jnp.float32)
    q_part = jnp.clip(2.0 * first, -10.0, 10.0)
    k_part = jnp.clip(second, -5.0, 5.0)
    return (q_part, k_part)


def draw_queries(key, part):
    return paired_draw(key)[0].astype(jnp.bfloat16)


def draw_video_keys(key, part):
    return paired_draw(key)[1].astype(jnp.bfloat16)


def draw_tile_radius(key, part):
    drawn = jax.random.randint(key, (3, TT_TILES, ROW_TILES, COL_TILES), 0, 2).astype(jnp.int32)
    return drawn.at[:, 0, 0, 0].set(1)


def block_scale(key, extent, cuts, least, high):
    def one(dim, parts):
        draws = jax.random.uniform(jax.random.fold_in(jax.random.fold_in(key, 6), dim), (parts,), jnp.float32, least / len(cuts), high / len(cuts))
        return jnp.repeat(jnp.exp(draws), extent[dim] // parts).reshape((-1,) + (1,) * (len(extent) - dim - 1))

    factor_of = one(*cuts[0])
    for cut in cuts[1:]:
        factor_of = factor_of * one(*cut)
    return factor_of


def noise(key, shape, deviation, most, cuts=(), kind=jnp.bfloat16):
    values = jax.random.normal(key, shape, jnp.float32) * deviation
    if len(cuts) > 0:
        values = block_scale(key, shape, cuts, -0.22, 0.18) * values
    return jnp.clip(values, min=-most, max=most).astype(kind)


def setup_inputs(seed: int = 0) -> dict:
    key_of = jax.random.split(jax.random.key(seed), 8)
    return {
        "queries": draw_queries(jax.random.fold_in(key_of[7], 71), 0),
        "video_keys": draw_video_keys(jax.random.fold_in(key_of[7], 71), 0),
        "video_values": noise(key_of[2], (FRAMES, HEIGHT, WIDTH, HEADS * HEAD), 1.0, 6.0, ((1, 4), (2, 4), (3, 2))),
        "text_keys": noise(key_of[3], (TEXT, HEADS * HEAD), 1.0, 5.0, ((1, 2),)),
        "text_values": noise(key_of[4], (TEXT, HEADS * HEAD), 1.0, 6.0, ((1, 2),)),
        "tile_radius": draw_tile_radius(jax.random.fold_in(key_of[7], 71), 0),
        "out_weight": noise(key_of[6], (HEADS * HEAD, D), 48 ** -0.5, 0.875, ((0, 2),)),
    }


def reference(queries, video_keys, video_values, text_keys, text_values, tile_radius, out_weight):
    n_frames, n_height, n_width, channels = queries.shape
    time_tiles = n_frames // TILE_T
    row_tiles = n_height // TILE_H
    col_tiles = n_width // TILE_W
    head_count = channels // HEAD
    factor = HEAD ** -0.5
    padding = ((0, 0), (TILE_H, TILE_H), (TILE_W, TILE_W), (0, 0))
    keys_padded = jnp.pad(video_keys, padding)
    values_padded = jnp.pad(video_values, padding)
    text_key32 = text_keys.astype(jnp.float32).reshape(-1, head_count, HEAD)
    text_val32 = text_values.astype(jnp.float32).reshape(-1, head_count, HEAD)

    def one_tile(tile_index):
        time_tile = tile_index // (row_tiles * col_tiles)
        row_tile = (tile_index // col_tiles) % row_tiles
        col_tile = tile_index % col_tiles
        zero = jnp.zeros((), jnp.int32)
        q_tile = lax.dynamic_slice(queries, (time_tile * TILE_T, row_tile * TILE_H, col_tile * TILE_W, zero), (TILE_T, TILE_H, TILE_W, channels))
        q_tile = q_tile.astype(jnp.float32).reshape(-1, head_count, HEAD)
        k_tile = lax.dynamic_slice(keys_padded, (zero, row_tile * TILE_H, col_tile * TILE_W, zero), (n_frames, 3 * TILE_H, 3 * TILE_W, channels))
        v_tile = lax.dynamic_slice(values_padded, (zero, row_tile * TILE_H, col_tile * TILE_W, zero), (n_frames, 3 * TILE_H, 3 * TILE_W, channels))
        k_tile = k_tile.astype(jnp.float32).reshape(-1, head_count, HEAD)
        v_tile = v_tile.astype(jnp.float32).reshape(-1, head_count, HEAD)
        key_time = jnp.arange(n_frames, dtype=jnp.int32) // TILE_T
        key_row = row_tile - 1 + jnp.arange(3 * TILE_H, dtype=jnp.int32) // TILE_H
        key_col = col_tile - 1 + jnp.arange(3 * TILE_W, dtype=jnp.int32) // TILE_W
        radius_here = tile_radius[:, time_tile, row_tile, col_tile]
        time_ok = jnp.abs(key_time - time_tile) <= radius_here[0]
        row_ok = (jnp.abs(key_row - row_tile) <= radius_here[1]) & (key_row >= 0) & (key_row < row_tiles)
        col_ok = (jnp.abs(key_col - col_tile) <= radius_here[2]) & (key_col >= 0) & (key_col < col_tiles)
        allowed = (time_ok[:, None, None] & row_ok[None, :, None] & col_ok[None, None, :]).reshape(-1)
        scores = jnp.einsum("qhd,khd->hqk", q_tile, k_tile) * factor
        text_scores = jnp.einsum("qhd,khd->hqk", q_tile, text_key32) * factor
        row_peak = jnp.maximum(jnp.max(jnp.where(allowed[None, None, :], scores, -jnp.inf), axis=2), jnp.max(text_scores, axis=2))[:, :, None]
        weights = jnp.where(allowed[None, None, :], jnp.exp(scores - row_peak), 0.0)
        text_weights = jnp.exp(text_scores - row_peak)
        row_total = jnp.sum(weights, axis=2) + jnp.sum(text_weights, axis=2)
        weights_low = lax.optimization_barrier(weights.astype(jnp.bfloat16)).astype(jnp.float32)
        text_low = lax.optimization_barrier(text_weights.astype(jnp.bfloat16)).astype(jnp.float32)
        numerator = jnp.einsum("hqk,khd->qhd", weights_low, v_tile) + jnp.einsum("hqk,khd->qhd", text_low, text_val32)
        result = (numerator / jnp.transpose(row_total)[:, :, None]).astype(jnp.bfloat16)
        return result.reshape(TILE_T, TILE_H, TILE_W, channels)

    tiles = lax.map(one_tile, jnp.arange(time_tiles * row_tiles * col_tiles, dtype=jnp.int32))
    tiles = tiles.reshape(time_tiles, row_tiles, col_tiles, TILE_T, TILE_H, TILE_W, channels)
    attended = jnp.transpose(tiles, (0, 3, 1, 4, 2, 5, 6)).reshape(-1, channels)
    group_width = channels // N_HD
    summed = jnp.zeros((attended.shape[0], out_weight.shape[1]), jnp.float32)
    for group in range(N_HD):
        portion = jnp.dot(attended[:, group * group_width:(group + 1) * group_width], out_weight[group * group_width:(group + 1) * group_width], preferred_element_type=jnp.float32)
        summed = summed + lax.optimization_barrier(portion.astype(jnp.bfloat16)).astype(jnp.float32)
    return summed.astype(jnp.bfloat16).reshape(n_frames, n_height, n_width, -1)
```

```python
import functools

import jax
import jax.numpy as jnp
from jax import lax
from jax.experimental import pallas as pl
from jax.experimental.pallas import tpu as pltpu
from jax.sharding import PartitionSpec as P

HEAD = 128
TILE_T = 6
TILE_H = 8
TILE_W = 8
TILE = TILE_T * TILE_H * TILE_W
LOG2E = 1.4426950408889634
SCALE = HEAD ** (-0.5) * LOG2E


def shift_pairs(axis):
    count = lax.axis_size(axis)
    forward = [(i, i + 1) for i in range(count - 1)]
    backward = [(target, source) for source, target in forward]
    return forward, backward


def attend_kernel(
    radius_ref, place_ref, q_ref, tk_ref, tv_ref, own_ref, low_ref, high_ref, left_ref, right_ref,
    o_ref, window, sems, peak_ref, total_ref, acc_ref,
):
    head, heads = pl.program_id(0), pl.num_programs(0)
    slot = lax.rem(head, 2)
    times, cols = q_ref.shape[1], q_ref.shape[2]

    def copies(which, where):
        inner = pl.ds(1, cols)
        pairs = (
            (low_ref.at[:, :, which], window.at[where, 0, inner]),
            (own_ref.at[:, :, which], window.at[where, 1, inner]),
            (high_ref.at[:, :, which], window.at[where, 2, inner]),
            (left_ref.at[:, :, which], window.at[where, :, 0]),
            (right_ref.at[:, :, which], window.at[where, :, cols + 1]),
        )
        return [
            pltpu.make_async_copy(source, target, sems.at[where, i])
            for i, (source, target) in enumerate(pairs)
        ]

    @pl.when(head == 0)
    def _():
        for copy in copies(head, slot):
            copy.start()

    @pl.when(head + 1 < heads)
    def _():
        for copy in copies(head + 1, 1 - slot):
            copy.start()

    for copy in copies(head, slot):
        copy.wait()

    row, last_row, col_base, last_col = (place_ref[i] for i in range(4))

    def scores_of(query, keys):
        dims = (((1,), (1,)), ((), ()))
        return lax.dot_general(query, keys, dims, preferred_element_type=jnp.float32) * SCALE

    def folded(weights):
        parts = [weights[:, i : i + HEAD] for i in range(0, weights.shape[1], HEAD)]
        result = parts[0]
        for part in parts[1:]:
            result = result + part
        return result

    def one_tile(tile, carry):
        a, e = tile // cols, lax.rem(tile, cols)
        query = q_ref[0, a, e]
        scores = scores_of(query, tk_ref[0])
        peak = jnp.max(scores, axis=1, keepdims=True)
        weights = jnp.exp2(scores - peak)
        peak_ref[...] = jnp.broadcast_to(peak, peak_ref.shape)
        total_ref[...] = folded(weights)
        acc_ref[...] = jnp.dot(
            weights.astype(jnp.bfloat16), tv_ref[0], preferred_element_type=jnp.float32
        )

        def absorb(keys, values):
            scores = scores_of(q_ref[0, a, e], keys)
            old = peak_ref[...]
            new = jnp.maximum(old, jnp.max(scores, axis=1, keepdims=True))
            shrink = jnp.exp2(old - new)
            weights = jnp.exp2(scores - new[:, :1])
            peak_ref[...] = new
            total_ref[...] = total_ref[...] * shrink + folded(weights)
            acc_ref[...] = acc_ref[...] * shrink + jnp.dot(
                weights.astype(jnp.bfloat16), values, preferred_element_type=jnp.float32
            )

        in_time = radius_ref[0, a, e]
        in_rows = radius_ref[1, a, e]
        in_cols = radius_ref[2, a, e]
        time_low = jnp.maximum(a - in_time, 0)
        time_high = jnp.minimum(a + in_time, times - 1)
        row_low = 1 - jnp.minimum(in_rows, row)
        row_high = 1 + jnp.minimum(in_rows, last_row - row)
        col_low = e + 1 - jnp.minimum(in_cols, col_base + e)
        col_high = e + 1 + jnp.minimum(in_cols, last_col - col_base - e)

        def over_rows(r, carry):
            def over_cols(c, carry):
                @pl.when(time_high - time_low + 1 == 2)
                def _():
                    keys = window[slot, r, c, 0, pl.ds(time_low, 2)].reshape(2 * TILE, HEAD)
                    values = window[slot, r, c, 1, pl.ds(time_low, 2)].reshape(2 * TILE, HEAD)
                    absorb(keys, values)

                @pl.when(time_high - time_low + 1 != 2)
                def _():
                    def over_times(b, carry):
                        absorb(window[slot, r, c, 0, b], window[slot, r, c, 1, b])
                        return carry

                    lax.fori_loop(time_low, time_high + 1, over_times, 0)

                return carry

            return lax.fori_loop(col_low, col_high + 1, over_cols, carry)

        lax.fori_loop(row_low, row_high + 1, over_rows, 0)
        row_total = jnp.sum(total_ref[...], axis=1, keepdims=True)
        o_ref[a, e] = (acc_ref[...] / row_total).astype(jnp.bfloat16)
        return carry

    lax.fori_loop(0, times * cols, one_tile, 0)


def attend(radius, place, q, tk, tv, own, low, high, left, right):
    heads, times, cols = q.shape[:3]
    text = tk.shape[1]
    smem = pl.BlockSpec(memory_space=pltpu.SMEM)
    anywhere = pl.BlockSpec(memory_space=pl.ANY)
    text_spec = pl.BlockSpec((1, text, HEAD), lambda h: (h, 0, 0))
    pairs = heads * times * cols * TILE * 10 * TILE
    return pl.pallas_call(
        attend_kernel,
        grid=(heads,),
        out_shape=jax.ShapeDtypeStruct((times, cols, TILE, heads * HEAD), jnp.bfloat16),
        in_specs=[
            smem,
            smem,
            pl.BlockSpec((1, times, cols, TILE, HEAD), lambda h: (h, 0, 0, 0, 0)),
            text_spec,
            text_spec,
        ]
        + [anywhere] * 5,
        out_specs=pl.BlockSpec((times, cols, TILE, HEAD), lambda h: (0, 0, 0, h)),
        scratch_shapes=[
            pltpu.VMEM((2, 3, cols + 2, 2, times, TILE, HEAD), jnp.bfloat16),
            pltpu.SemaphoreType.DMA((2, 5)),
            pltpu.VMEM((TILE, HEAD), jnp.float32),
            pltpu.VMEM((TILE, HEAD), jnp.float32),
            pltpu.VMEM((TILE, HEAD), jnp.float32),
        ],
        compiler_params=pltpu.CompilerParams(
            dimension_semantics=("arbitrary",), vmem_limit_bytes=60000 * 1024
        ),
        cost_estimate=pl.CostEstimate(
            flops=4 * pairs * HEAD, bytes_accessed=heads * 6 * 2**20, transcendentals=pairs
        ),
    )(radius, place, q, tk, tv, own, low, high, left, right)


def by_tile(block):
    n_frames, _, across, channels = block.shape
    times, cols, heads = n_frames // TILE_T, across // TILE_W, channels // HEAD
    block = block.reshape(times, TILE_T, TILE_H, cols, TILE_W, heads, HEAD)
    return block.transpose(3, 5, 0, 1, 2, 4, 6).reshape(cols, heads, times, TILE, HEAD)


def text_heads(block):
    return block.reshape(block.shape[0], -1, HEAD).transpose(1, 0, 2)


def shards(queries, video_keys, video_values, text_keys, text_values, tile_radius, out_weight):
    n_frames, height, across, channels = queries.shape
    times, cols = n_frames // TILE_T, across // TILE_W
    heads = channels // HEAD
    step = 2 if heads % 2 == 0 else 1
    groups = lax.axis_size("hd")
    mine = lax.axis_index("hd")
    width = out_weight.shape[1] // groups
    row_up, row_down = shift_pairs("ha")
    col_up, col_down = shift_pairs("wa")
    place = jnp.stack(
        [
            lax.axis_index("ha"),
            jnp.int32(lax.axis_size("ha") - 1),
            lax.axis_index("wa") * cols,
            jnp.int32(lax.axis_size("wa") * cols - 1),
        ]
    ).astype(jnp.int32)
    radius = tile_radius.reshape(3, times, cols)

    def turned(array, shift):
        return lax.ppermute(array, "hd", [(i, (i + shift) % groups) for i in range(groups)])

    owns, lows, highs = [], [], []
    for first in range(0, heads, step):
        part = slice(first * HEAD, (first + step) * HEAD)
        own = jnp.stack([by_tile(video_keys[..., part]), by_tile(video_values[..., part])], axis=1)
        owns.append(own)
        lows.append(lax.ppermute(own, "ha", row_up))
        highs.append(lax.ppermute(own, "ha", row_down))

    sheets = []
    for shift in range(groups):
        start = lax.rem(mine + shift, groups) * width
        sheet = lax.dynamic_slice_in_dim(out_weight, start, width, 1)
        sheets.append(sheet if shift == 0 else turned(sheet, shift))

    pieces = [[] for _ in range(groups)]
    for index, first in enumerate(range(0, heads, step)):
        part = slice(first * HEAD, (first + step) * HEAD)
        own, low, high = owns[index], lows[index], highs[index]
        left = lax.ppermute(jnp.stack([low[-1], own[-1], high[-1]]), "wa", col_up)
        right = lax.ppermute(jnp.stack([low[0], own[0], high[0]]), "wa", col_down)
        q = by_tile(queries[..., part]).transpose(1, 2, 0, 3, 4)
        tk, tv = text_heads(text_keys[:, part]), text_heads(text_values[:, part])
        attended = attend(radius, place, q, tk, tv, own, low, high, left, right)
        pieces[0].append(attended)
        for shift in range(1, groups):
            pieces[shift].append(turned(attended, shift))

    mixture = jnp.concatenate([piece for group in pieces for piece in group], axis=3)
    weight = jnp.concatenate(sheets, axis=0)
    projected = jnp.dot(
        mixture.reshape(-1, mixture.shape[3]), weight, preferred_element_type=jnp.float32
    ).astype(jnp.bfloat16)
    projected = projected.reshape(times, cols, TILE_T, TILE_H, TILE_W, width)
    return projected.transpose(0, 2, 3, 1, 4, 5).reshape(n_frames, height, across, width)


def solution(mesh):
    placed = (
        P(None, "ha", "wa", "hd"),
        P(None, "ha", "wa", "hd"),
        P(None, "ha", "wa", "hd"),
        P(None, "hd"),
        P(None, "hd"),
        P(None, None, "ha", "wa"),
        P("hd", None),
    )
    return jax.shard_map(
        shards, mesh=mesh, in_specs=placed, out_specs=P(None, "ha", "wa", "hd"), check_vma=False
    )
```
